256 devices in a mesh: mp: 32 (over x, z), dp: 8 (over y, core).
Axes of the slice: x: 4, y: 4, z: 8, core: 2. Of those that a mesh axis runs over, the one named last changes fastest.
Arguments:
- tables: bfloat16 [20, 65536, 128], P(None, 'mp'), may hold values from -3 to 3
- block_rows: int32 [16384, 128], P(('mp', 'dp')), may hold values from 0 to 2047
- block_slots: int32 [16384, 128], P(('mp', 'dp')), may hold values from 0 to 127
- block_table: int32 [16384], P(('mp', 'dp')), may hold values from 0 to 19
- block_peer: int32 [16384, 1], P(('mp', 'dp')), may hold values from 0 to 31; in each aligned block of 64 rows (0 to 63, 64 to 127, ...) at most 4 rows name the same one
- block_len: int32 [16384], P(('mp', 'dp')), may hold values from 1 to 128
- block_count: int32 [256], P(('mp', 'dp')), may hold values from 1 to 64, as said below
- cross_in: bfloat16 [4, 2560, 256], P(None, 'dp'), may hold values from -0.23632812 to 0.23632812
- cross_mix: bfloat16 [4, 256, 256], replicated, may hold values from -0.5625 to 0.5625
- cross_out: bfloat16 [4, 256, 2560], P(None, None, 'dp'), may hold values from -0.375 to 0.375
- cross_bias: float32 [4, 2560], replicated, may hold values from -3 to 3
- gate_weight: bfloat16 [4, 2560], replicated, may hold values from -0.47265625 to 0.47265625
Outputs:
- crossed: bfloat16 [32768, 2560], P(('mp', 'dp'))
The draws below stay inside these ranges and needn't reach their ends.
Inputs may be any that keep to these rules, and one draw needn't show every extreme that they name: `block_peer`: in the 64 blocks of one device no destination is named by more than 4 blocks, a bound that the blocks of some device reach. The live blocks of a device are its first block_count blocks; some device has exactly 64. Entries of a block at positions below its block_len are live. `block_rows`: A row index within the device's own shard of the table. `block_slots`: A sample of the destination device.
All inputs are finite; a program needn't handle non-finite values.
Results may differ from the reference program's by a relative error of at most 0.0059.
Values may be sent and summed in bfloat16 or wider, within the bound.
No kernel may reach another device: no remote copies, remote signals or barrier semaphores. Data moves between devices by JAX's collectives and lax.ppermute only.
A program may use at most 128 MiB of HBM per device.

```python
import math
import jax
import jax.numpy as jnp
import numpy as np
from jax import lax

WIDTH = 128
TABLES = 20
ROWS_DEV = 2048
BLOCK = 128
NBLK = 64
B_DEV = 128
RANK = 256
EXPERTS = 4
D = 2560
CAP = 4
N_MP = 32
N_DP = 8


def draw_block_count(key, part):
    devices = N_MP * N_DP
    heavy = jax.random.randint(jax.random.fold_in(key, 11), (devices,), 0, 8) == 0
    high = jax.random.randint(jax.random.fold_in(key, 12), (devices,), NBLK // 2, NBLK + 1)
    low = jax.random.randint(jax.random.fold_in(key, 13), (devices,), max(1, NBLK // 8), NBLK // 2 + 1)
    counts = jnp.where(heavy, high, low)
    chosen = jax.random.randint(jax.random.fold_in(key, 14), (), 0, devices)
    return counts.at[chosen].set(NBLK).astype(jnp.int32)


def touch_ends(values, own_key, least, largest):
    extent = values.shape
    place = [jax.random.randint(jax.random.fold_in(own_key, axis), (), 0, extent[axis]) for axis in range(len(extent))]
    values = values.at[tuple(place)].set(least)
    longest = extent.index(max(extent))
    place[longest] = (place[longest] + 1) % extent[longest]
    return values.at[tuple(place)].set(largest)


def block_levels(key, extent, cuts, smallest, top_value):
    loudness = 1.0
    for dim, blocks in cuts:
        draws = jax.random.uniform(jax.random.fold_in(jax.random.fold_in(key, 6), dim), (blocks,), jnp.float32, smallest / len(cuts), top_value / len(cuts))
        loudness = loudness * jnp.repeat(jnp.exp(draws), extent[dim] // blocks).reshape((-1,) + (1,) * (len(extent) - 1 - dim))
    return loudness


def routed_block(key, own, number, rows, amount, top, bound, slope):
    order = jax.random.permutation(key, amount)
    packed, common = load_shares(amount, rows * top, bound, slope, True), load_shares(amount, rows * top, bound, slope, False)
    places = jnp.arange(amount)

    def named(tallies, rotation):
        used = int((tallies > 0).sum())
        fixed = max(1, used // 4)
        passed = fixed + (places - fixed + rotation * (used - fixed)) % max(1, amount - fixed)
        return jnp.zeros((amount,), jnp.int32).at[order[jnp.where(places < fixed, places, passed)]].set(jnp.asarray(tallies, jnp.int32))

    tallies = jnp.where(number % 4 == 0, named(packed, number // 4), named(common, number - number // 4 - 1))
    mixed = jax.random.permutation(jax.random.fold_in(own, 3), amount)
    donor, receiver = mixed[0:amount // 2 * 2:2], mixed[1:amount // 2 * 2:2]
    margin = jnp.minimum(tallies[donor] - 1, bound - tallies[receiver]) // 2
    margin = jnp.where((donor == order[0]) | (receiver == order[0]) | (tallies[receiver] == 0), 0, jnp.maximum(margin, 0))
    passed = jax.random.randint(jax.random.fold_in(own, 4), (amount // 2,), 0, 1 << 20) % (margin + 1)
    tallies = tallies.at[donor].add(-passed).at[receiver].add(passed)
    labels = jnp.searchsorted(jnp.cumsum(tallies), jnp.arange(rows * top), side="right").astype(jnp.int32)
    grid = labels.reshape(top, rows).T
    grid = grid[jax.random.permutation(jax.random.fold_in(own, 1), rows)]
    rotation = jax.random.randint(jax.random.fold_in(own, 2), (rows, 1), 0, top)
    return jnp.take_along_axis(grid, (jnp.arange(top)[None, :] + rotation) % top, axis=1)


def load_shares(count, total, reach, skew, full):
    weights = [(1 << 20) // math.isqrt(standing ** skew) + 1 for standing in range(1, count + 1)]
    largest = reach if full else min(reach, max(-(-total // count), total * weights[0] // sum(weights)))
    least = 1 if total - largest >= count - 1 else 0
    given, surplus = [largest] + [least] * (count - 1), total - largest - least * (count - 1)
    while surplus > 0:
        free = [i for i in range(1, count) if given[i] < largest] or [i for i in range(1, count) if given[i] < reach]
        whole, budget = sum([weights[i] for i in free]), surplus
        for i in free:
            extra = min(reach - given[i], max(1, budget * weights[i] // whole), surplus)
            given[i] = given[i] + extra
            surplus = surplus - extra
    return np.array(given)


def normal_values(stream_key, dims, deviation, limit, shards=(), kind=jnp.bfloat16):
    level = block_levels(stream_key, dims, shards, -0.22, 0.18) if shards else 1.0
    values = jax.random.normal(stream_key, dims, jnp.float32) * deviation * level
    return jnp.minimum(jnp.maximum(values, -limit), limit).astype(kind)


def setup_inputs(seed: int = 0) -> dict:
    key_list = jax.random.split(jax.random.key(seed), 13)
    tables = normal_values(key_list[0], (TABLES, ROWS_DEV * N_MP, WIDTH), 0.5, 3.0, ((1, 32),))
    block_rows = touch_ends(jax.random.randint(key_list[1], (N_MP * N_DP * NBLK, BLOCK), 0, ROWS_DEV), jax.random.fold_in(key_list[1], 1), 0, ROWS_DEV - 1).astype(jnp.int32)
    block_slots = touch_ends(jax.random.randint(key_list[2], (N_MP * N_DP * NBLK, BLOCK), 0, B_DEV), jax.random.fold_in(key_list[2], 1), 0, B_DEV - 1).astype(jnp.int32)
    block_table = touch_ends(jax.random.randint(key_list[3], (N_MP * N_DP * NBLK,), 0, TABLES), jax.random.fold_in(key_list[3], 1), 0, TABLES - 1).astype(jnp.int32)
    block_peer_keys = jax.random.split(jax.random.fold_in(key_list[4], 1), (N_MP * N_DP * NBLK) // NBLK)
    block_peer_turns = jax.random.permutation(jax.random.fold_in(key_list[4], 3), (N_MP * N_DP * NBLK) // NBLK)
    block_peer = jax.vmap(lambda own, number: routed_block(jax.random.fold_in(key_list[4], 2), own, number, NBLK, N_MP, 1, CAP, 2))(block_peer_keys, block_peer_turns).reshape((N_MP * N_DP * NBLK, 1))
    block_len = touch_ends(jax.random.randint(key_list[5], (N_MP * N_DP * NBLK,), 1, BLOCK + 1), jax.random.fold_in(key_list[5], 1), 1, BLOCK).astype(jnp.int32)
    block_count = draw_block_count(jax.random.fold_in(key_list[12], 71), 0)
    cross_in = normal_values(key_list[7], (EXPERTS, D, RANK), (2.0 / D ** 0.5), 0.23632812, ((1, 8),))
    cross_mix = normal_values(key_list[8], (EXPERTS, RANK, RANK), (1.5 / RANK ** 0.5), 0.5625)
    cross_out = normal_values(key_list[9], (EXPERTS, RANK, D), RANK ** -0.5, 0.375, ((2, 8),))
    cross_bias = normal_values(key_list[10], (EXPERTS, D), 0.5, 3.0, (), jnp.float32)
    gate_weight = normal_values(key_list[11], (EXPERTS, D), (4.0 / D ** 0.5), 0.47265625)
    return {"tables": tables, "block_rows": block_rows, "block_slots": block_slots, "block_table": block_table, "block_peer": block_peer, "block_len": block_len, "block_count": block_count, "cross_in": cross_in, "cross_mix": cross_mix, "cross_out": cross_out, "cross_bias": cross_bias, "gate_weight": gate_weight}


def reference(tables, block_rows, block_slots, block_table, block_peer, block_len, block_count, cross_in, cross_mix, cross_out, cross_bias, gate_weight):
    devices = N_MP * N_DP
    rows_all = block_rows.reshape(devices, NBLK, BLOCK)
    slots_all = block_slots.reshape(devices, NBLK, BLOCK)
    table_all = block_table.reshape(devices, NBLK)
    peer_all = block_peer.reshape(devices, NBLK)
    length_all = block_len.reshape(devices, NBLK)
    entries = jnp.arange(BLOCK, dtype=jnp.int32)
    blocks = jnp.arange(NBLK, dtype=jnp.int32)

    def one_device(index, total):
        shard = index // N_DP
        group = index % N_DP
        live = (blocks[:, None] < block_count[index]) & (entries[None, :] < length_all[index][:, None])
        table_ids = jnp.broadcast_to(table_all[index][:, None], (NBLK, BLOCK)).astype(jnp.int32)
        peer_ids = jnp.broadcast_to(peer_all[index][:, None], (NBLK, BLOCK)).astype(jnp.int32)
        row_ids = (rows_all[index] + shard * ROWS_DEV).astype(jnp.int32)
        values = tables[table_ids, row_ids].astype(jnp.float32) * live[:, :, None].astype(jnp.float32)
        partial_value = jnp.zeros((N_MP, TABLES, B_DEV, WIDTH), jnp.float32)
        partial_value = partial_value.at[peer_ids, table_ids, slots_all[index]].add(values)
        rounded = lax.optimization_barrier(partial_value.astype(jnp.bfloat16)).astype(jnp.float32)
        return total.at[:, group].add(rounded)

    total = lax.fori_loop(0, devices, one_device, jnp.zeros((N_MP, N_DP, TABLES, B_DEV, WIDTH), jnp.float32))
    embedded = total.transpose(0, 1, 3, 2, 4).reshape(devices * B_DEV, TABLES * WIDTH).astype(jnp.bfloat16)
    gate = jax.nn.sigmoid(jnp.dot(embedded, gate_weight.T, preferred_element_type=jnp.float32))
    weighted = jnp.zeros(embedded.shape, jnp.float32)
    for expert in range(EXPERTS):
        hidden = jnp.tanh(jnp.dot(embedded, cross_in[expert], preferred_element_type=jnp.float32)).astype(jnp.bfloat16)
        mixed = jnp.tanh(jnp.dot(hidden, cross_mix[expert], preferred_element_type=jnp.float32)).astype(jnp.bfloat16)
        expand = jnp.dot(mixed, cross_out[expert], preferred_element_type=jnp.float32) + cross_bias[expert][None, :]
        weighted = weighted + gate[:, expert][:, None] * expand
    base = embedded.astype(jnp.float32)
    return (base + base * weighted).astype(jnp.bfloat16)
```

```python
import jax
import jax.numpy as jnp
from jax import lax
from jax.experimental import pallas as pl
from jax.experimental.pallas import tpu as pltpu
from jax.sharding import PartitionSpec as P

UNIT = 16
LANES = 128


def block_meta(block_slots, block_table, block_peer, block_len, count, peers, tables):
    blocks, width = block_slots.shape
    ids = jnp.arange(blocks, dtype=jnp.int32)
    live = ids < count
    lens = jnp.where(live, block_len, 0)
    entry_live = jnp.arange(width, dtype=jnp.int32)[None, :] < lens[:, None]
    slots = jnp.where(entry_live, block_slots, -1)
    samples = jnp.arange(LANES, dtype=jnp.int32)
    hit = slots[:, :, None] == samples[None, None, :]
    present = jnp.any(hit, axis=1)
    upper = (samples[:, None] < samples[None, :]).astype(jnp.bfloat16)
    rank = jnp.dot(present.astype(jnp.bfloat16), upper, preferred_element_type=jnp.float32).astype(jnp.int32)
    rows = jnp.sum(present.astype(jnp.int32), axis=1)
    rank_slot = jnp.where(present, rank, -1)
    rank_entry = jnp.max(jnp.where(hit, rank[:, None, :], -1), axis=2)
    units = (rows + UNIT - 1) // UNIT
    same = (block_peer[:, None] == block_peer[None, :]) & live[None, :] & (ids[None, :] < ids[:, None])
    position = jnp.sum(same.astype(jnp.int32), axis=1)
    start = jnp.sum(jnp.where(same, units[None, :], 0), axis=1)
    total = jnp.max(jnp.where(live, start + units, 0))
    key = jnp.where(live, block_table, tables) * blocks + ids
    place = jnp.sum((key[None, :] < key[:, None]).astype(jnp.int32), axis=1)
    order = jnp.sum(jnp.where(place[None, :] == ids[:, None], ids[None, :], 0), axis=1)
    bounds = jnp.sum(
        (live[None, :] & (block_table[None, :] < jnp.arange(blocks, dtype=jnp.int32)[:, None])).astype(jnp.int32), axis=1
    )
    return dict(live=live, lens=lens, rank_slot=rank_slot, rank_entry=rank_entry, units=units, position=position,
                start=start, total=total, order=order, bounds=bounds)


def pack_kernel(meta, rows, rank, tables_hbm, out, stage, wide, picked, sems):
    tables, rows_dev, width = tables_hbm.shape

    def copy(t):
        return pltpu.make_async_copy(tables_hbm.at[t], stage.at[t], sems.at[t])

    for t in range(tables):
        copy(t).start()
    picked[...] = jnp.zeros_like(picked)

    def clear(p, carry):
        out[p] = jnp.zeros(out.shape[1:], out.dtype)
        return carry

    lax.fori_loop(0, out.shape[0], clear, 0)
    unit_rows = lax.broadcasted_iota(jnp.int32, (LANES, LANES), 0)

    def one_block(k, carry):
        b = meta[0, k]
        length = meta[1, b]
        units = meta[2, b]
        first = meta[3, b]
        peer = meta[4, b]

        def eight(i, c):
            base = pl.multiple_of(i * 8, 8)
            got = [wide[pl.ds(rows[b, base + j], 1), :] for j in range(8)]
            picked[pl.ds(base, 8), :] = jnp.concatenate(got, axis=0)
            return c

        lax.fori_loop(0, (length + 7) // 8, eight, 0)
        choose = (rank[pl.ds(b, 1), :] == unit_rows).astype(jnp.float32).astype(jnp.bfloat16)
        packed = jnp.dot(choose, picked[...].astype(jnp.bfloat16), preferred_element_type=jnp.float32)
        packed = packed.astype(jnp.bfloat16)
        for u in range(LANES // UNIT):
            @pl.when(u < units)
            def _():
                out[peer, pl.ds(pl.multiple_of((first + u) * UNIT, UNIT), UNIT), :] = packed[u * UNIT:(u + 1) * UNIT]
        return carry

    def one_table(t, carry):
        copy(t).wait()
        lo = meta[5, t]
        hi = meta[5, t + 1]

        @pl.when(hi > lo)
        def _():
            def widen(i, c):
                at = pl.multiple_of(i * 256, 256)
                wide[pl.ds(at, 256), :] = stage[t, pl.ds(at, 256), :].astype(jnp.float32)
                return c

            lax.fori_loop(0, rows_dev // 256, widen, 0)
            lax.fori_loop(lo, hi, one_block, 0)

        return carry

    lax.fori_loop(0, tables, one_table, 0)


def pack(meta, rows, rank, tables, peers, cap_rows):
    count, rows_dev, width = tables.shape
    return pl.pallas_call(
        pack_kernel,
        out_shape=jax.ShapeDtypeStruct((peers, cap_rows, width), jnp.bfloat16),
        in_specs=[
            pl.BlockSpec(memory_space=pltpu.SMEM),
            pl.BlockSpec(memory_space=pltpu.SMEM),
            pl.BlockSpec(memory_space=pltpu.VMEM),
            pl.BlockSpec(memory_space=pltpu.HBM),
        ],
        out_specs=pl.BlockSpec(memory_space=pltpu.VMEM),
        scratch_shapes=[
            pltpu.VMEM((count, rows_dev, width), jnp.bfloat16),
            pltpu.VMEM((rows_dev, width), jnp.float32),
            pltpu.VMEM((LANES, width), jnp.float32),
            pltpu.SemaphoreType.DMA((count,)),
        ],
        compiler_params=pltpu.CompilerParams(vmem_limit_bytes=40 * 2**20),
        name="pack_rows",
    )(meta, rows, rank, tables)


def unpack_kernel(meta, rank, rows, out):
    tables = out.shape[1] // LANES
    last = rows.shape[0] - LANES
    row_ids = lax.broadcasted_iota(jnp.int32, (LANES, LANES), 0)

    def one_table(t, carry):
        lo = meta[1, t]
        hi = meta[1, t + 1]

        def one_pair(i, acc):
            picks, parts = [], []
            for j in range(2):
                k = lo + 2 * i + j
                b = meta[0, jnp.minimum(k, hi - 1)]
                first = meta[2, b]
                base = jnp.minimum(first, last)
                skip = jnp.where(k < hi, first - base, 2 * LANES)
                picks.append(rank[pl.ds(b, 1), :] + skip == row_ids)
                parts.append(rows[pl.ds(pl.multiple_of(base, UNIT), LANES), :])
            choose = jnp.concatenate(picks, axis=0).astype(jnp.float32).astype(jnp.bfloat16)
            return acc + lax.dot_general(
                choose, jnp.concatenate(parts, axis=0), (((0,), (0,)), ((), ())), preferred_element_type=jnp.float32
            )

        total = lax.fori_loop(0, (hi - lo + 1) // 2, one_pair, jnp.zeros((LANES, LANES), jnp.float32))
        out[:, pl.ds(pl.multiple_of(t * LANES, LANES), LANES)] = total.astype(out.dtype)
        return carry

    lax.fori_loop(0, tables, one_table, 0)


def unpack(meta, rank, rows, tables):
    return pl.pallas_call(
        unpack_kernel,
        out_shape=jax.ShapeDtypeStruct((LANES, tables * LANES), jnp.bfloat16),
        in_specs=[
            pl.BlockSpec(memory_space=pltpu.SMEM),
            pl.BlockSpec(memory_space=pltpu.VMEM),
            pl.BlockSpec(memory_space=pltpu.VMEM),
        ],
        out_specs=pl.BlockSpec(memory_space=pltpu.VMEM),
        compiler_params=pltpu.CompilerParams(vmem_limit_bytes=40 * 2**20),
        name="unpack_rows",
    )(meta, rank, rows)


def make_header(m, block_table, block_peer, peers):
    blocks, width = m["rank_slot"].shape
    extra = jnp.stack([m["live"].astype(jnp.int32), block_table, m["start"]], axis=1)
    values = jnp.concatenate(
        [m["rank_slot"] + 1, extra, jnp.zeros((blocks, width - 3), jnp.int32)], axis=1
    ).astype(jnp.bfloat16)
    target = jnp.where(m["live"], block_peer * 4 + m["position"], -1)
    place = (target[None, :] == jnp.arange(4 * peers, dtype=jnp.int32)[:, None]).astype(jnp.bfloat16)
    spread = jnp.dot(place, values, preferred_element_type=jnp.float32).astype(jnp.bfloat16)
    return spread.reshape(peers, 4, 2 * width)


def read_header(header, tables):
    peers, each, wide = header.shape
    flat = header.reshape(peers * each, wide).astype(jnp.int32)
    rank = flat[:, :LANES] - 1
    live = flat[:, LANES] > 0
    table = jnp.where(live, flat[:, LANES + 1], tables)
    start = flat[:, LANES + 2]
    ids = jnp.arange(peers * each, dtype=jnp.int32)
    key = table * (peers * each) + ids
    place = jnp.sum((key[None, :] < key[:, None]).astype(jnp.int32), axis=1)
    order = jnp.sum(jnp.where(place[None, :] == ids[:, None], ids[None, :], 0), axis=1)
    bounds = jnp.sum((table[None, :] < ids[:, None]).astype(jnp.int32), axis=1)
    return rank, order, bounds, start


CAPS = (8, 12, 16, 18, 20, 22, 24, 28, 32)


def on_device(
    tables,
    block_rows,
    block_slots,
    block_table,
    block_peer,
    block_len,
    block_count,
    cross_in,
    cross_mix,
    cross_out,
    cross_bias,
    gate_weight,
):
    peers = lax.axis_size("mp")
    table_count = tables.shape[0]
    down = lax.all_gather(cross_in, "dp", axis=1, tiled=True)
    up = lax.all_gather(jnp.swapaxes(cross_out, 1, 2), "dp", axis=1, tiled=True)
    peer = block_peer[:, 0]
    m = block_meta(block_slots, block_table, peer, block_len, block_count[0], peers, table_count)
    header = lax.all_to_all(make_header(m, block_table, peer, peers), "mp", split_axis=0, concat_axis=0, tiled=True)
    most = lax.pmax(m["total"], ("mp", "dp"))
    table = jnp.stack([m["order"], m["lens"], m["units"], m["start"], peer, m["bounds"]])
    packed = pack(table, block_rows, m["rank_entry"], tables, peers, 4 * LANES)
    rank, order, bounds, start = read_header(header, table_count)

    def exchange(cap):
        def run(packed, rank, order, bounds, start):
            rows = cap * UNIT
            got = lax.all_to_all(packed[:, :rows], "mp", split_axis=0, concat_axis=0, tiled=True)
            source = jnp.arange(start.shape[0], dtype=jnp.int32) // 4
            meta = jnp.stack([order, bounds, source * rows + start * UNIT])
            return unpack(meta, rank, got.reshape(peers * rows, LANES), table_count)

        return run

    level = sum((most > cap).astype(jnp.int32) for cap in CAPS[:-1])
    embedded = lax.switch(level, [exchange(cap) for cap in CAPS], packed, rank, order, bounds, start)

    gate = jax.nn.sigmoid(jnp.dot(embedded, gate_weight.T, preferred_element_type=jnp.float32))
    projected = jnp.einsum("bn,enr->ebr", embedded, down, preferred_element_type=jnp.float32)
    hidden = jnp.tanh(projected).astype(jnp.bfloat16)
    mixed = jnp.tanh(
        jnp.einsum("ebr,erq->ebq", hidden, cross_mix, preferred_element_type=jnp.float32)
    ).astype(jnp.bfloat16)
    grown = jnp.einsum("ebr,enr->ebn", mixed, up, preferred_element_type=jnp.float32)
    grown = grown + cross_bias[:, None, :]
    weighted = jnp.sum(gate.T[:, :, None] * grown, axis=0)
    base = embedded.astype(jnp.float32)
    return (base + base * weighted).astype(jnp.bfloat16)


def solution(mesh):
    in_specs = (
        P(None, "mp", None),
        P(("mp", "dp"), None),
        P(("mp", "dp"), None),
        P(("mp", "dp")),
        P(("mp", "dp"), None),
        P(("mp", "dp")),
        P(("mp", "dp")),
        P(None, "dp", None),
        P(),
        P(None, None, "dp"),
        P(),
        P(),
    )
    return jax.shard_map(
        on_device, mesh=mesh, in_specs=in_specs, out_specs=P(("mp", "dp"), None), check_vma=False
    )
```
